32 devices in a mesh: fsdp: 8 (over z, y), tp: 4 (over x, core).
Axes of the slice: x: 2, y: 2, z: 4, core: 2. Of those that a mesh axis runs over, the one named last changes fastest.
Arguments:
- layer_input: bfloat16 [2, 8192, 768], P(None, ('fsdp', 'tp')), may hold values from -6 to 6
- out_grad: bfloat16 [2, 8192, 768], P(None, ('fsdp', 'tp')), may hold values from -6 to 6
- ln1_gain: float32 [768], replicated, may hold values from 0.5 to 1.5
- ln1_bias: float32 [768], replicated, may hold values from -3 to 3
- w_query: bfloat16 [768, 768], P('fsdp', 'tp'), may hold values from -0.21875 to 0.21875
- w_key: bfloat16 [768, 768], P('fsdp', 'tp'), may hold values from -0.21875 to 0.21875
- w_value: bfloat16 [768, 768], P('fsdp', 'tp'), may hold values from -0.21875 to 0.21875
- conv_query: float32 [3, 768], replicated, may hold values from -3 to 3
- conv_key: float32 [3, 768], replicated, may hold values from -3 to 3
- conv_value: float32 [3, 768], replicated, may hold values from -3 to 3
- w_out: bfloat16 [768, 768], P('tp', 'fsdp'), may hold values from -1.25 to 1.25
- ln2_gain: float32 [768], replicated, may hold values from 0.5 to 1.5
- ln2_bias: float32 [768], replicated, may hold values from -3 to 3
- w_up: bfloat16 [768, 3072], P('fsdp', 'tp'), may hold values from -0.21875 to 0.21875
- up_bias: float32 [3072], replicated, may hold values from -3 to 3
- w_down: bfloat16 [3072, 768], P('tp', 'fsdp'), may hold values from -0.109375 to 0.109375
- down_bias: float32 [768], replicated, may hold values from -3 to 3
Outputs:
- layer_out: bfloat16 [2, 8192, 768], P(None, ('fsdp', 'tp'))
- in_grad: bfloat16 [2, 8192, 768], P(None, ('fsdp', 'tp'))
- ln1_gain_grad: float32 [768], replicated
- ln1_bias_grad: float32 [768], replicated
- w_query_grad: float32 [768, 768], P('fsdp', 'tp')
- w_key_grad: float32 [768, 768], P('fsdp', 'tp')
- w_value_grad: float32 [768, 768], P('fsdp', 'tp')
- conv_query_grad: float32 [3, 768], replicated
- conv_key_grad: float32 [3, 768], replicated
- conv_value_grad: float32 [3, 768], replicated
- w_out_grad: float32 [768, 768], P('tp', 'fsdp')
- ln2_gain_grad: float32 [768], replicated
- ln2_bias_grad: float32 [768], replicated
- w_up_grad: float32 [768, 3072], P('fsdp', 'tp')
- up_bias_grad: float32 [3072], replicated
- w_down_grad: float32 [3072, 768], P('tp', 'fsdp')
- down_bias_grad: float32 [768], replicated
The draws below stay inside these ranges and needn't reach their ends.
All inputs are finite; a program needn't handle non-finite values.
Results may differ from the reference program's by a relative error of at most 0.02.
Values may be sent and summed in bfloat16 or wider, within the bound.
A program may use at most 192 MiB of HBM per device.

```python
import jax
import jax.numpy as jnp
from jax import lax

HEADS = 12
HEAD_DIM = 64
D = 768
FF = 3072
SEQ = 1024
MB = 2
KBLOCK = 256
QBLOCK = 512
TOKENS = 8192
N_FSDP = 8


def block_scale(own_key, shape, shards, low, largest):
    level = 1.0
    for axis_at, blocks in shards:
        draws = jax.random.uniform(jax.random.fold_in(jax.random.fold_in(own_key, 6), axis_at), (blocks,), jnp.float32, low / len(shards), largest / len(shards))
        level = level * jnp.repeat(jnp.exp(draws), shape[axis_at] // blocks).reshape((-1,) + (1,) * (len(shape) - 1 - axis_at))
    return level


def bell_draw(stream_key, shape, spread, bound, pieces=(), kind=jnp.bfloat16):
    values = spread * jax.random.normal(stream_key, shape, jnp.float32)
    if pieces:
        values = values * block_scale(stream_key, shape, pieces, -0.22, 0.18)
    return jnp.clip(values, -bound, bound).astype(kind)


def setup_inputs(seed: int = 0) -> dict:
    key_of = jax.random.split(jax.random.key(seed), 18)
    return {
        "layer_input": bell_draw(key_of[0], (MB, TOKENS, D), 1.0, 6.0, ((1, 32),)),
        "out_grad": bell_draw(key_of[1], (MB, TOKENS, D), 1.0, 6.0, ((1, 32),)),
        "ln1_gain": jnp.clip(1.0 + 0.1 * jax.random.normal(key_of[2], (D,), jnp.float32), 0.5, 1.5),
        "ln1_bias": bell_draw(key_of[3], (D,), 0.3, 3.0, (), jnp.float32),
        "w_query": bell_draw(key_of[4], (D, D), D ** -0.5, 0.21875, ((0, 8), (1, 4))),
        "w_key": bell_draw(key_of[5], (D, D), D ** -0.5, 0.21875, ((0, 8), (1, 4))),
        "w_value": bell_draw(key_of[6], (D, D), D ** -0.5, 0.21875, ((0, 8), (1, 4))),
        "conv_query": bell_draw(key_of[7], (3, D), 0.6, 3.0, (), jnp.float32),
        "conv_key": bell_draw(key_of[8], (3, D), 0.6, 3.0, (), jnp.float32),
        "conv_value": bell_draw(key_of[9], (3, D), 0.6, 3.0, (), jnp.float32),
        "w_out": bell_draw(key_of[10], (D, D), (D // 32) ** -0.5, 1.25, ((0, 4), (1, 8))),
        "ln2_gain": jnp.clip(1.0 + 0.1 * jax.random.normal(key_of[11], (D,), jnp.float32), 0.5, 1.5),
        "ln2_bias": bell_draw(key_of[12], (D,), 0.3, 3.0, (), jnp.float32),
        "w_up": bell_draw(key_of[13], (D, FF), D ** -0.5, 0.21875, ((0, 8), (1, 4))),
        "up_bias": bell_draw(key_of[14], (FF,), 0.5, 3.0, (), jnp.float32),
        "w_down": bell_draw(key_of[15], (FF, D), FF ** -0.5, 0.109375, ((0, 4), (1, 8))),
        "down_bias": bell_draw(key_of[16], (D,), 0.5, 3.0, (), jnp.float32),
    }


@jax.custom_vjp
def low(v):
    return lax.optimization_barrier(v.astype(jnp.bfloat16)).astype(jnp.float32)

@jax.custom_vjp
def low_back(v):
    return v

def low_keep(v):
    return (low(v), None)

def low_pass(kept, grad):
    return (grad,)

def back_keep(v):
    return (v, None)

def back_low(kept, grad):
    return (low(grad),)
low.defvjp(low_keep, low_pass)
low_back.defvjp(back_keep, back_low)
EPS = 1e-05
MASKED = -1e+30

def project(left, right):
    return jnp.dot(left, right, precision=lax.Precision.HIGHEST)

def layer_norm(values, gain, shift):
    center = values - lax.optimization_barrier(jnp.mean(values, axis=-1, keepdims=True))
    inverse = lax.rsqrt(lax.optimization_barrier(jnp.mean(center * center, axis=-1, keepdims=True)) + EPS)
    return center * inverse * gain + shift

def shifted(values, steps):
    width = values.shape[1]
    return jnp.concatenate([jnp.zeros((steps, width), values.dtype), values[:-steps]], axis=0)

def causal_conv(values, kernel):
    return kernel[0] * values + kernel[1] * shifted(values, 1) + kernel[2] * shifted(values, 2)

def attention(query_mix, key_mix, value_mix):
    length = query_mix.shape[0]
    queries = query_mix.reshape(length // QBLOCK, QBLOCK, HEADS, HEAD_DIM)
    keys = key_mix.reshape(length, HEADS, HEAD_DIM)
    values = value_mix.reshape(length, HEADS, HEAD_DIM)
    key_block = jnp.arange(length, dtype=jnp.int32) // KBLOCK

    def one_block(pair):
        query_part, number = pair
        row_block = (number * QBLOCK + jnp.arange(QBLOCK, dtype=jnp.int32)) // KBLOCK
        allowed = key_block[None, :] <= row_block[:, None]
        scores = jnp.einsum('qhd,khd->hqk', query_part, keys, precision=lax.Precision.HIGHEST) * HEAD_DIM ** (-0.5)
        scores = low_back(jnp.where(allowed[None], scores, MASKED))
        weights = low(jax.nn.softmax(scores, axis=-1))
        return jnp.einsum('hqk,khd->qhd', weights, values, precision=lax.Precision.HIGHEST)
    mixed = lax.map(jax.checkpoint(one_block), (queries, jnp.arange(length // QBLOCK, dtype=jnp.int32)))
    return mixed.reshape(length, HEADS * HEAD_DIM)

def layer(rows, params):
    ln1_gain, ln1_bias, w_query, w_key, w_value, conv_query, conv_key, conv_value, w_out, ln2_gain, ln2_bias, w_up, up_bias, w_down, down_bias = params
    hidden_one = low(layer_norm(rows, ln1_gain, ln1_bias))
    query = low_back(project(hidden_one, w_query))
    key = low_back(project(hidden_one, w_key))
    value = low_back(project(hidden_one, w_value))
    query_mix = low(causal_conv(query, conv_query))
    key_mix = low(causal_conv(key, conv_key))
    value_mix = low(causal_conv(value, conv_value))
    mixed = low(low_back(attention(query_mix, key_mix, value_mix)))
    attn_rows = low_back(project(mixed, w_out))
    resid = rows + attn_rows
    hidden_two = low(layer_norm(resid, ln2_gain, ln2_bias))
    pre_act = low_back(project(hidden_two, w_up) + up_bias)
    relu_part = jnp.maximum(pre_act, 0.0)
    activ = low(relu_part * relu_part)
    ffn_rows = low_back(project(activ, w_down))
    return resid + ffn_rows + down_bias

def reference(layer_input, out_grad, ln1_gain, ln1_bias, w_query, w_key, w_value, conv_query, conv_key, conv_value, w_out, ln2_gain, ln2_bias, w_up, up_bias, w_down, down_bias):
    params = tuple((item.astype(jnp.float32) for item in (ln1_gain, ln1_bias, w_query, w_key, w_value, conv_query, conv_key, conv_value, w_out, ln2_gain, ln2_bias, w_up, up_bias, w_down, down_bias)))
    inputs = layer_input.astype(jnp.float32).reshape(MB * N_FSDP, SEQ, D)
    cotangents = out_grad.astype(jnp.float32).reshape(MB * N_FSDP, SEQ, D)

    def one_sequence(totals, pair):
        rows, grad_rows = pair
        result, pull = jax.vjp(layer, rows, params)
        grad_input, grad_params = pull(grad_rows)
        totals = jax.tree.map(jnp.add, totals, grad_params)
        return (totals, (result.astype(jnp.bfloat16), grad_input.astype(jnp.bfloat16)))
    start_totals = jax.tree.map(jnp.zeros_like, params)
    totals, (results, input_grads) = lax.scan(one_sequence, start_totals, (inputs, cotangents))
    return (results.reshape(MB, N_FSDP * SEQ, D), input_grads.reshape(MB, N_FSDP * SEQ, D), totals[0], totals[1], totals[2], totals[3], totals[4], totals[5], totals[6], totals[7], totals[8], totals[9], totals[10], totals[11], totals[12], totals[13], totals[14])
```

```python
import functools

import jax
import jax.numpy as jnp
from jax import lax
from jax.experimental import pallas as pl
from jax.experimental.pallas import tpu as pltpu
from jax.sharding import PartitionSpec as P

HEAD_DIM = 64
D = 768
FF = 3072
KBLOCK = 256
QBLOCK = 512
EPS = 1e-05
MASKED = -1e30
MESH = pl.DeviceIdType.MESH
BF = jnp.bfloat16
F32 = jnp.float32
VMEM_LIMIT = 60 << 20


def place(ny):
    f = lax.axis_index("fsdp")
    t = lax.axis_index("tp")
    return f, t, f // ny, f % ny, t // 2, t % 2


def remote(src, dst, send, recv, dev):
    return pltpu.make_async_remote_copy(
        src_ref=src, dst_ref=dst, send_sem=send, recv_sem=recv, device_id=dev, device_id_type=MESH
    )


def greet(peers):
    bar = pltpu.get_barrier_semaphore()
    for p in peers:
        pl.semaphore_signal(bar, inc=1, device_id=p, device_id_type=MESH)
    pl.semaphore_wait(bar, len(peers))


def gather_kernel(nz, ny, split, w_ref, x_ref, g_ref, W, X, G, zs, zr, hs, hr, acts, actr, local_sem):
    f, t, z, y, xx, c = place(ny)
    nch, R = w_ref.shape[0], w_ref.shape[1]
    xpeer = (f, (1 - xx) * 2 + c)
    ypeer = (z * ny + (1 - y), t)
    cpeer = (f, xx * 2 + 1 - c)
    zp = [((z + d) % nz) * ny + y for d in range(1, nz)]
    greet([xpeer, ypeer, cpeer] + [(q, t) for q in zp])
    other = 1 - xx
    blk = xx * 2 + c
    oblk = other * 2 + c
    ax = remote(x_ref.at[other], X.at[blk], acts.at[0], actr.at[0], xpeer)
    ax.start()
    zc = []
    for ch in range(nch):
        row = []
        for d in range(nz - 1):
            cp = remote(w_ref.at[ch], W.at[ch, xx, z, y], zs.at[ch, d], zr.at[ch, d], (zp[d], t))
            cp.start()
            row.append(cp)
        zc.append(row)
    agc = remote(g_ref.at[other], G.at[blk], acts.at[1], actr.at[1], xpeer)
    agc.start()
    loc = []
    pairs = [(x_ref.at[xx], X.at[blk]), (g_ref.at[xx], G.at[blk])]
    pairs += [(w_ref.at[ch], W.at[ch, xx, z, y]) for ch in range(nch)]
    for i, (s, d) in enumerate(pairs):
        cp = pltpu.make_async_copy(s, d, local_sem.at[i])
        cp.start()
        loc.append(cp)
    c0 = remote(x_ref.at[xx], X.at[blk], acts.at[2], actr.at[2], cpeer)
    c0.start()
    c1 = remote(g_ref.at[xx], G.at[blk], acts.at[3], actr.at[3], cpeer)
    c1.start()
    for cp in loc:
        cp.wait()
    ax.wait()
    c2 = remote(X.at[oblk], X.at[oblk], acts.at[4], actr.at[4], cpeer)
    c2.start()
    A = pl.ds(0, split)
    B = pl.ds(split, R - split)
    st2 = []
    st3 = []
    for ch in range(nch):
        for cp in zc[ch]:
            cp.wait()
        wa = W.at[ch, xx, :, y, A]
        wb = W.at[ch, xx, :, y, B]
        a = remote(wa, wa, hs.at[ch, 0, 0], hr.at[ch, 0, 0], ypeer)
        b = remote(wb, wb, hs.at[ch, 0, 1], hr.at[ch, 0, 1], xpeer)
        a.start()
        b.start()
        st2.append((a, b))
    agc.wait()
    c3 = remote(G.at[oblk], G.at[oblk], acts.at[5], actr.at[5], cpeer)
    c3.start()
    for ch in range(nch):
        st2[ch][0].wait()
        wa = W.at[ch, xx, :, :, A]
        a = remote(wa, wa, hs.at[ch, 1, 0], hr.at[ch, 1, 0], xpeer)
        a.start()
        st2[ch][1].wait()
        wb = W.at[ch, :, :, y, B]
        b = remote(wb, wb, hs.at[ch, 1, 1], hr.at[ch, 1, 1], ypeer)
        b.start()
        st3 += [a, b]
    for cp in st3 + [c0, c1, c2, c3]:
        cp.wait()


def gather(w, x, g, nf, split):
    ny = 2
    nz = nf // ny
    nch, R, C = w.shape
    V = pl.BlockSpec(memory_space=pltpu.VMEM)
    S = pltpu.SemaphoreType.DMA
    rows, dm = x.shape[1:]
    return pl.pallas_call(
        functools.partial(gather_kernel, nz, ny, split),
        out_shape=[
            jax.ShapeDtypeStruct((nch, 2, nz, ny, R, C), w.dtype),
            jax.ShapeDtypeStruct((4, rows, dm), x.dtype),
            jax.ShapeDtypeStruct((4, rows, dm), x.dtype),
        ],
        in_specs=[V, V, V],
        out_specs=[V, V, V],
        scratch_shapes=[
            S((nch, nz - 1)),
            S((nch, nz - 1)),
            S((nch, 2, 2)),
            S((nch, 2, 2)),
            S((6,)),
            S((6,)),
            S((2 + nch,)),
        ],
        compiler_params=pltpu.CompilerParams(
            collective_id=0, has_side_effects=True, vmem_limit_bytes=VMEM_LIMIT
        ),
    )(w, x, g)


def settle_kernel(nz, ny, split, *refs):
    grads = refs[:3]
    vec, lo, ig, out, vout, lo_out, ig_out = refs[3:10]
    ra1, ra2, rb1, rb2, r3, s2, vsend, vr, ss, sr, zs, zr, acts, actr, vs, vrs, loc = refs[10:]
    f, t, z, y, xx, c = place(ny)
    nch = 3
    R = out.shape[1]
    xpeer = (f, (1 - xx) * 2 + c)
    ypeer = (z * ny + (1 - y), t)
    cpeer = (f, xx * 2 + 1 - c)
    zp = [((z + d) % nz) * ny + y for d in range(1, nz)]
    greet([xpeer, ypeer, cpeer] + [(q, t) for q in zp])
    other = 1 - xx
    A = pl.ds(0, split)
    B = pl.ds(split, R - split)
    o1 = remote(lo.at[other], lo_out.at[xx], acts.at[0], actr.at[0], xpeer)
    o2 = remote(ig.at[other], ig_out.at[xx], acts.at[1], actr.at[1], xpeer)
    l1 = pltpu.make_async_copy(lo.at[xx], lo_out.at[xx], loc.at[0])
    l2 = pltpu.make_async_copy(ig.at[xx], ig_out.at[xx], loc.at[1])
    steps = [xpeer, cpeer, ypeer]
    v0 = remote(vec, vr.at[0], vs.at[0], vrs.at[0], xpeer)
    v0.start()
    st1 = []
    for ch in range(nch):
        a = remote(grads[ch].at[other, :, :, A], ra1.at[ch], ss.at[ch, 0, 0], sr.at[ch, 0, 0], xpeer)
        b = remote(grads[ch].at[:, :, 1 - y, B], rb1.at[ch], ss.at[ch, 0, 1], sr.at[ch, 0, 1], ypeer)
        a.start()
        b.start()
        st1.append((a, b))
    o1.start()
    o2.start()
    l1.start()
    l2.start()
    st2 = []
    for ch in range(nch):
        a, b = st1[ch]
        a.wait()
        for zi in range(nz):
            ra1[ch, zi, 1 - y] = (
                ra1[ch, zi, 1 - y].astype(F32) + grads[ch][xx, zi, 1 - y, A].astype(F32)
            ).astype(BF)
        a2 = remote(ra1.at[ch, :, 1 - y], ra2.at[ch], ss.at[ch, 1, 0], sr.at[ch, 1, 0], ypeer)
        a2.start()
        b.wait()
        for zi in range(nz):
            rb1[ch, other, zi] = (
                rb1[ch, other, zi].astype(F32) + grads[ch][other, zi, y, B].astype(F32)
            ).astype(BF)
        b2 = remote(rb1.at[ch, other], rb2.at[ch], ss.at[ch, 1, 1], sr.at[ch, 1, 1], xpeer)
        b2.start()
        st2.append((a2, b2))
    v0.wait()
    vsend[0] = vec[...] + vr[0]
    v1 = remote(vsend.at[0], vr.at[1], vs.at[1], vrs.at[1], cpeer)
    v1.start()
    v1.wait()
    vsend[1] = vsend[0] + vr[1]
    v2 = remote(vsend.at[1], vr.at[2], vs.at[2], vrs.at[2], ypeer)
    v2.start()
    v2.wait()
    vsend[2] = vsend[1] + vr[2]
    vz = []
    for d in range(nz - 1):
        cp = remote(vsend.at[2], vr.at[3 + nz - 2 - d], vs.at[3 + d], vrs.at[3 + nz - 2 - d], (zp[d], t))
        cp.start()
        vz.append(cp)
    st3 = []
    for ch in range(nch):
        a2, b2 = st2[ch]
        a2.wait()
        for zi in range(nz):
            s2[ch, zi, A] = (
                ra1[ch, zi, y].astype(F32) + grads[ch][xx, zi, y, A].astype(F32) + ra2[ch, zi].astype(F32)
            ).astype(BF)
        b2.wait()
        for zi in range(nz):
            s2[ch, zi, B] = (
                rb1[ch, xx, zi].astype(F32) + grads[ch][xx, zi, y, B].astype(F32) + rb2[ch, zi].astype(F32)
            ).astype(BF)
        row = []
        for d in range(nz - 1):
            k = nz - 2 - d
            cp = remote(s2.at[ch, (z + 1 + d) % nz], r3.at[ch, k], zs.at[ch, d], zr.at[ch, k], (zp[d], t))
            cp.start()
            row.append(cp)
        st3.append(row)
    for cp in vz:
        cp.wait()
    total = vsend[2]
    for d in range(nz - 1):
        total = total + vr[3 + d]
    vout[...] = total
    for ch in range(nch):
        for cp in st3[ch]:
            cp.wait()
        total = s2[ch, z].astype(F32)
        for d in range(nz - 1):
            total = total + r3[ch, d].astype(F32)
        out[ch] = total
    o1.wait()
    o2.wait()
    l1.wait()
    l2.wait()


def settle(grads, vec, lo, ig, nf, split):
    ny = 2
    nz = nf // ny
    _, _, _, R, C = grads[0].shape
    nch = 3
    V = pl.BlockSpec(memory_space=pltpu.VMEM)
    S = pltpu.SemaphoreType.DMA
    M = pltpu.VMEM
    return pl.pallas_call(
        functools.partial(settle_kernel, nz, ny, split),
        out_shape=[
            jax.ShapeDtypeStruct((nch, R, C), F32),
            jax.ShapeDtypeStruct(vec.shape, F32),
            jax.ShapeDtypeStruct(lo.shape, lo.dtype),
            jax.ShapeDtypeStruct(ig.shape, ig.dtype),
        ],
        in_specs=[V] * 6,
        out_specs=[V] * 4,
        scratch_shapes=[
            M((nch, nz, ny, split, C), BF),
            M((nch, nz, split, C), BF),
            M((nch, 2, nz, R - split, C), BF),
            M((nch, nz, R - split, C), BF),
            M((nch, nz - 1, R, C), BF),
            M((nch, nz, R, C), BF),
            M((3,) + vec.shape, F32),
            M((3 + nz - 1,) + vec.shape, F32),
            S((nch, 2, 2)),
            S((nch, 2, 2)),
            S((nch, nz - 1)),
            S((nch, nz - 1)),
            S((2,)),
            S((2,)),
            S((3 + nz - 1,)),
            S((3 + nz - 1,)),
            S((2,)),
        ],
        compiler_params=pltpu.CompilerParams(
            collective_id=1, has_side_effects=True, vmem_limit_bytes=VMEM_LIMIT
        ),
    )(*grads, vec, lo, ig)


def normalize(values, gain, shift):
    center = values - jnp.mean(values, axis=-1, keepdims=True)
    inverse = lax.rsqrt(jnp.mean(center * center, axis=-1, keepdims=True) + EPS)
    unit = center * inverse
    return (unit, inverse, unit * gain + shift)


def normalize_back(grad_rows, unit, inverse, gain):
    scaled = grad_rows * gain
    return inverse * (
        scaled
        - jnp.mean(scaled, axis=-1, keepdims=True)
        - unit * jnp.mean(scaled * unit, axis=-1, keepdims=True)
    )


def shifted(values, steps):
    return jnp.concatenate(
        [jnp.zeros((steps, values.shape[1]), values.dtype), values[:-steps]], axis=0
    )


def advanced(values, steps):
    return jnp.concatenate(
        [values[steps:], jnp.zeros((steps, values.shape[1]), values.dtype)], axis=0
    )


def conv_apply(values, kernel):
    return kernel[0] * values + kernel[1] * shifted(values, 1) + kernel[2] * shifted(values, 2)


def conv_back(grad_mix, values, kernel):
    grad_values = (
        kernel[0] * grad_mix + kernel[1] * advanced(grad_mix, 1) + kernel[2] * advanced(grad_mix, 2)
    )
    kernel_grad = jnp.stack(
        [
            jnp.sum(grad_mix * values, axis=0),
            jnp.sum(grad_mix * shifted(values, 1), axis=0),
            jnp.sum(grad_mix * shifted(values, 2), axis=0),
        ]
    )
    return (grad_values, kernel_grad)


def block_probs(q_ref, k_ref, lse_ref, h, blk):
    keys = (blk + 1) * KBLOCK
    q = q_ref[h, pl.ds(blk * KBLOCK, KBLOCK), :]
    k = k_ref[h, pl.ds(0, keys), :]
    s = lax.dot_general(q, k, (((1,), (1,)), ((), ())), preferred_element_type=F32)
    return s * HEAD_DIM ** (-0.5)


def attend_kernel(q_ref, k_ref, v_ref, o_ref, lse_ref):
    nblk = q_ref.shape[1] // KBLOCK
    for blk in range(nblk):
        rows = pl.ds(blk * KBLOCK, KBLOCK)
        s = block_probs(q_ref, k_ref, lse_ref, 0, blk)
        top = jnp.max(s, axis=-1, keepdims=True)
        lse = top + jnp.log(jnp.sum(jnp.exp(s - top), axis=-1, keepdims=True))
        p = jnp.exp(s - lse).astype(BF)
        v = v_ref[0, pl.ds(0, (blk + 1) * KBLOCK), :]
        o_ref[0, rows, :] = jnp.dot(p, v, preferred_element_type=F32).astype(BF)
        lse_ref[0, rows, :] = lse


def attend(q, k, v):
    heads, rows, hd = q.shape
    spec = pl.BlockSpec((1, rows, hd), lambda h: (h, 0, 0))
    lspec = pl.BlockSpec((1, rows, 1), lambda h: (h, 0, 0))
    return pl.pallas_call(
        attend_kernel,
        grid=(heads,),
        out_shape=[
            jax.ShapeDtypeStruct((heads, rows, hd), BF),
            jax.ShapeDtypeStruct((heads, rows, 1), F32),
        ],
        in_specs=[spec] * 3,
        out_specs=[spec, lspec],
        compiler_params=pltpu.CompilerParams(vmem_limit_bytes=40 << 20),
    )(q, k, v)


def attend_back_kernel(q_ref, k_ref, v_ref, do_ref, lse_ref, dq_ref, dk_ref, dv_ref):
    nblk = q_ref.shape[1] // KBLOCK
    dk_ref[...] = jnp.zeros_like(dk_ref)
    dv_ref[...] = jnp.zeros_like(dv_ref)
    scale = HEAD_DIM ** (-0.5)
    for blk in range(nblk):
        rows = pl.ds(blk * KBLOCK, KBLOCK)
        keys = pl.ds(0, (blk + 1) * KBLOCK)
        s = block_probs(q_ref, k_ref, lse_ref, 0, blk)
        pe = jnp.exp(s - lse_ref[0, rows, :])
        do = do_ref[0, rows, :]
        v = v_ref[0, keys, :]
        dp = lax.dot_general(do, v, (((1,), (1,)), ((), ())), preferred_element_type=F32)
        inner = jnp.sum(pe * dp, axis=-1, keepdims=True)
        ds = (pe * (dp - inner)).astype(BF)
        dq_ref[0, rows, :] = jnp.dot(ds, k_ref[0, keys, :], preferred_element_type=F32) * scale
        q = q_ref[0, rows, :]
        dk_ref[0, keys, :] += (
            lax.dot_general(ds, q, (((0,), (0,)), ((), ())), preferred_element_type=F32) * scale
        )
        dv_ref[0, keys, :] += lax.dot_general(
            pe.astype(BF), do, (((0,), (0,)), ((), ())), preferred_element_type=F32
        )


def attend_back(q, k, v, do, lse):
    heads, rows, hd = q.shape
    spec = pl.BlockSpec((1, rows, hd), lambda h: (h, 0, 0))
    lspec = pl.BlockSpec((1, rows, 1), lambda h: (h, 0, 0))
    shape = jax.ShapeDtypeStruct((heads, rows, hd), F32)
    return pl.pallas_call(
        attend_back_kernel,
        grid=(heads,),
        out_shape=[shape] * 3,
        in_specs=[spec] * 4 + [lspec],
        out_specs=[spec] * 3,
        compiler_params=pltpu.CompilerParams(vmem_limit_bytes=40 << 20),
    )(q, k, v, do, lse)


def swap(value):
    n = lax.axis_size("tp")
    return lax.ppermute(value, "tp", [(i, i ^ 1) for i in range(n)])


def local(
    layer_input,
    out_grad,
    ln1_gain,
    ln1_bias,
    w_query,
    w_key,
    w_value,
    conv_query,
    conv_key,
    conv_value,
    w_out,
    ln2_gain,
    ln2_bias,
    w_up,
    up_bias,
    w_down,
    down_bias,
):
    nf = lax.axis_size("fsdp")
    rank = lax.axis_index("tp")
    core = rank % 2
    depth, width = w_query.shape
    units = w_up.shape[1]
    heads = width // HEAD_DIM
    span = layer_input.shape[1]
    rows = 4 * span
    padded = -(-depth // 32) * 32
    split = max(16, padded // 48 * 16)
    pack = jnp.stack(
        [jnp.concatenate([w_query, w_key, w_value, w_out.T], axis=1), w_up, w_down.T]
    )
    if padded != depth:
        pack = jnp.pad(pack, ((0, 0), (0, padded - depth), (0, 0)))
    W, X, G = gather(pack, layer_input, out_grad, nf, split)
    W = W.reshape(3, 2, nf, padded, D)[:, :, :, :depth].reshape(3, 2, D, D)
    x = X.reshape(rows, D).astype(F32)
    g = G.reshape(rows, D)

    def mine(vector, size):
        return jnp.stack(
            [
                lax.dynamic_slice_in_dim(vector, (2 * i + core) * size, size, vector.ndim - 1)
                for i in range(2)
            ],
            axis=-2,
        )

    kernels = [mine(v, width).reshape(3, 2 * width) for v in (conv_query, conv_key, conv_value)]
    bias_up = mine(up_bias, units)

    def half(value):
        v = value.reshape(2, 2, span, D)
        return (
            lax.dynamic_index_in_dim(v, core, 1, keepdims=False),
            lax.dynamic_index_in_dim(v, 1 - core, 1, keepdims=False),
        )

    unit_one, inverse_one, normed_one = normalize(x, ln1_gain, ln1_bias)
    hidden_one = normed_one.astype(BF)
    w_qkv = W[0, :, :, : 3 * width]
    w_o = W[0, :, :, 3 * width :]
    projs = []
    for i in range(3):
        wi = jnp.concatenate([W[0, j, :, i * width : (i + 1) * width] for j in range(2)], axis=1)
        projs.append(jnp.dot(hidden_one, wi, preferred_element_type=F32))

    def heads_first(v):
        return v.reshape(rows, 2 * heads, HEAD_DIM).transpose(1, 0, 2)

    def heads_last(v):
        return v.transpose(1, 0, 2).reshape(rows, 2 * width)

    mixes = [heads_first(conv_apply(p, k).astype(BF)) for p, k in zip(projs, kernels)]
    mixed, lse = attend(*mixes)
    attn_rows = heads_last(mixed)
    full_o = jnp.concatenate([w_o[0], w_o[1]], axis=1)
    part = jnp.einsum("tc,dc->td", attn_rows, full_o, preferred_element_type=F32).astype(BF)
    resid = x + part.astype(F32) + swap(part).astype(F32)
    unit_two, inverse_two, normed_two = normalize(resid, ln2_gain, ln2_bias)
    hidden_two = normed_two.astype(BF)
    relus, activs = [], []
    y_part = 0.0
    for j in range(2):
        pre = jnp.dot(hidden_two, W[1, j], preferred_element_type=F32) + bias_up[j]
        r = jnp.maximum(pre, 0.0)
        relus.append(r.astype(BF))
        activs.append((r * r).astype(BF))
        y_part = y_part + jnp.einsum("tu,du->td", activs[j], W[2, j], preferred_element_type=F32)
    y_own, y_other = half(y_part.astype(BF))
    resid_own, _ = half(resid)
    layer_out = (
        resid_own + (y_own.astype(F32) + swap(y_other).astype(F32)) + down_bias
    ).astype(BF)
    g32 = g.astype(F32)
    bias_down_grad = jnp.sum(g32, axis=0)
    dh2 = 0.0
    up_grads, down_grads, bias_up_grads = [], [], []
    for j in range(2):
        da = jnp.einsum("td,du->tu", g, W[2, j], preferred_element_type=F32)
        dz = (da * 2.0 * relus[j].astype(F32)).astype(BF)
        bias_up_grads.append(jnp.sum(dz.astype(F32), axis=0))
        down_grads.append(jnp.einsum("td,tu->du", g, activs[j], preferred_element_type=F32).astype(BF))
        up_grads.append(
            jnp.einsum("td,tu->du", hidden_two, dz, preferred_element_type=F32).astype(BF)
        )
        dh2 = dh2 + jnp.einsum("tu,du->td", dz, W[1, j], preferred_element_type=F32)
    dh2 = dh2.astype(BF)
    dh2 = dh2.astype(F32) + swap(dh2).astype(F32)
    gain_two = jnp.sum(dh2 * unit_two, axis=0)
    shift_two = jnp.sum(dh2, axis=0)
    dx1 = g32 + normalize_back(dh2, unit_two, inverse_two, ln2_gain)
    dattn = dx1.astype(BF)
    out_grad_t = jnp.einsum("td,tc->dc", dattn, attn_rows, preferred_element_type=F32).astype(BF)
    dmixed = jnp.einsum("td,dc->tc", dattn, full_o, preferred_element_type=F32).astype(BF)
    dmixes = attend_back(*mixes, heads_first(dmixed), lse)
    dh1 = 0.0
    attn_grads, taps = [], []
    for i in range(3):
        dv, tap = conv_back(heads_last(dmixes[i]), projs[i], kernels[i])
        taps.append(tap)
        dv = dv.astype(BF)
        attn_grads.append(
            jnp.einsum("td,tc->dc", hidden_one, dv, preferred_element_type=F32).astype(BF)
        )
        wi = jnp.concatenate([W[0, j, :, i * width : (i + 1) * width] for j in range(2)], axis=1)
        dh1 = dh1 + jnp.einsum("tc,dc->td", dv, wi, preferred_element_type=F32)
    own, rest = half(dh1.astype(BF))
    dh1 = own.astype(F32) + swap(rest).astype(F32)
    unit_own, _ = half(unit_one)
    inverse_own = lax.dynamic_index_in_dim(
        inverse_one.reshape(2, 2, span, 1), core, 1, keepdims=False
    )
    dx1_own, _ = half(dx1)
    gain_one = jnp.sum(dh1 * unit_own, axis=(0, 1))
    shift_one = jnp.sum(dh1, axis=(0, 1))
    in_grad = (dx1_own + normalize_back(dh1, unit_own, inverse_own, ln1_gain)).astype(BF)
    ch0 = jnp.stack(
        [
            jnp.concatenate(
                [v[:, j * width : (j + 1) * width] for v in attn_grads + [out_grad_t]], axis=1
            )
            for j in range(2)
        ]
    )

    def slabs(v):
        v = v.reshape(2, nf // 2, 2, depth, D)
        if padded != depth:
            v = jnp.pad(v, ((0, 0),) * 3 + ((0, padded - depth), (0, 0)))
        return v

    grads = [slabs(ch0), slabs(jnp.stack(up_grads)), slabs(jnp.stack(down_grads))]

    def spread(v, size):
        full = jnp.zeros(v.shape[:-2] + (4 * size,), F32)
        for i in range(2):
            full = lax.dynamic_update_slice_in_dim(
                full, v[..., i, :], (2 * i + core) * size, full.ndim - 1
            )
        return full

    first = (core == 0).astype(F32)
    pieces = [
        gain_one,
        shift_one,
        *[spread(tp.reshape(3, 2, width), width).reshape(-1) for tp in taps],
        first * gain_two,
        first * shift_two,
        spread(jnp.stack(bias_up_grads), units),
        first * bias_down_grad,
    ]
    vec = jnp.concatenate(pieces)
    count = vec.shape[0]
    lines = -(-count // 1024) * 8
    vec = jnp.pad(vec, (0, lines * 128 - count)).reshape(lines, 128)
    out, vec, lo, ig = settle(grads, vec, layer_out, in_grad, nf, split)
    vec = vec.reshape(-1)
    sums = []
    at = 0
    for p in pieces:
        sums.append(vec[at : at + p.shape[0]])
        at += p.shape[0]
    out = out[:, :depth]
    qg, kg, vg, og = [out[0][:, i * width : (i + 1) * width] for i in range(4)]
    return (
        lo,
        ig,
        sums[0],
        sums[1],
        qg,
        kg,
        vg,
        sums[2].reshape(3, D),
        sums[3].reshape(3, D),
        sums[4].reshape(3, D),
        og.T,
        sums[5],
        sums[6],
        out[1],
        sums[7],
        out[2].T,
        sums[8],
    )


def solution(mesh):
    rowsharded = P(None, ("fsdp", "tp"), None)
    return jax.shard_map(
        local,
        mesh=mesh,
        in_specs=(
            rowsharded,
            rowsharded,
            P(),
            P(),
            P("fsdp", "tp"),
            P("fsdp", "tp"),
            P("fsdp", "tp"),
            P(),
            P(),
            P(),
            P("tp", "fsdp"),
            P(),
            P(),
            P("fsdp", "tp"),
            P(),
            P("tp", "fsdp"),
            P(),
        ),
        out_specs=(
            rowsharded,
            rowsharded,
            P(),
            P(),
            P("fsdp", "tp"),
            P("fsdp", "tp"),
            P("fsdp", "tp"),
            P(),
            P(),
            P(),
            P("tp", "fsdp"),
            P(),
            P(),
            P("fsdp", "tp"),
            P(),
            P("tp", "fsdp"),
            P(),
        ),
        check_vma=False,
    )
```

```python
import functools

import jax
import jax.numpy as jnp
from jax import lax
from jax.experimental import pallas as pl
from jax.experimental.pallas import tpu as pltpu
from jax.sharding import PartitionSpec as P

HEAD_DIM = 64
D = 768
FF = 3072
KBLOCK = 256
EPS = 1e-05
MESH = pl.DeviceIdType.MESH
BF = jnp.bfloat16
F32 = jnp.float32
VMEM_LIMIT = 60 << 20


def place(ny):
    f = lax.axis_index("fsdp")
    t = lax.axis_index("tp")
    return f, t, f // ny, f % ny, t // 2, t % 2


def remote(src, dst, send, recv, dev):
    return pltpu.make_async_remote_copy(
        src_ref=src, dst_ref=dst, send_sem=send, recv_sem=recv, device_id=dev, device_id_type=MESH
    )


def greet(peers):
    bar = pltpu.get_barrier_semaphore()
    for p in peers:
        pl.semaphore_signal(bar, inc=1, device_id=p, device_id_type=MESH)
    pl.semaphore_wait(bar, len(peers))


def gather_kernel(nz, ny, split, w_ref, x_ref, g_ref, W, X, G, zs, zr, hs, hr, acts, actr, local_sem):
    f, t, z, y, xx, c = place(ny)
    nch, R = w_ref.shape[0], w_ref.shape[1]
    xpeer = (f, (1 - xx) * 2 + c)
    ypeer = (z * ny + (1 - y), t)
    cpeer = (f, xx * 2 + 1 - c)
    zp = [((z + d) % nz) * ny + y for d in range(1, nz)]
    greet([xpeer, ypeer, cpeer] + [(q, t) for q in zp])
    other = 1 - xx
    blk = xx * 2 + c
    oblk = other * 2 + c
    ax = remote(x_ref.at[other], X.at[blk], acts.at[0], actr.at[0], xpeer)
    ax.start()
    zc = []
    for ch in range(nch):
        row = []
        for d in range(nz - 1):
            cp = remote(w_ref.at[ch], W.at[ch, xx, z, y], zs.at[ch, d], zr.at[ch, d], (zp[d], t))
            cp.start()
            row.append(cp)
        zc.append(row)
    agc = remote(g_ref.at[other], G.at[blk], acts.at[1], actr.at[1], xpeer)
    agc.start()
    loc = []
    pairs = [(x_ref.at[xx], X.at[blk]), (g_ref.at[xx], G.at[blk])]
    pairs += [(w_ref.at[ch], W.at[ch, xx, z, y]) for ch in range(nch)]
    for i, (s, d) in enumerate(pairs):
        cp = pltpu.make_async_copy(s, d, local_sem.at[i])
        cp.start()
        loc.append(cp)
    c0 = remote(x_ref.at[xx], X.at[blk], acts.at[2], actr.at[2], cpeer)
    c0.start()
    c1 = remote(g_ref.at[xx], G.at[blk], acts.at[3], actr.at[3], cpeer)
    c1.start()
    for cp in loc:
        cp.wait()
    ax.wait()
    c2 = remote(X.at[oblk], X.at[oblk], acts.at[4], actr.at[4], cpeer)
    c2.start()
    A = pl.ds(0, split)
    B = pl.ds(split, R - split)
    st2 = []
    st3 = []
    for ch in range(nch):
        for cp in zc[ch]:
            cp.wait()
        wa = W.at[ch, xx, :, y, A]
        wb = W.at[ch, xx, :, y, B]
        a = remote(wa, wa, hs.at[ch, 0, 0], hr.at[ch, 0, 0], ypeer)
        b = remote(wb, wb, hs.at[ch, 0, 1], hr.at[ch, 0, 1], xpeer)
        a.start()
        b.start()
        st2.append((a, b))
    agc.wait()
    c3 = remote(G.at[oblk], G.at[oblk], acts.at[5], actr.at[5], cpeer)
    c3.start()
    for ch in range(nch):
        st2[ch][0].wait()
        wa = W.at[ch, xx, :, :, A]
        a = remote(wa, wa, hs.at[ch, 1, 0], hr.at[ch, 1, 0], xpeer)
        a.start()
        st2[ch][1].wait()
        wb = W.at[ch, :, :, y, B]
        b = remote(wb, wb, hs.at[ch, 1, 1], hr.at[ch, 1, 1], ypeer)
        b.start()
        st3 += [a, b]
    for cp in st3 + [c0, c1, c2, c3]:
        cp.wait()


def gather(w, x, g, nf, split):
    ny = 2
    nz = nf // ny
    nch, R, C = w.shape
    V = pl.BlockSpec(memory_space=pltpu.VMEM)
    S = pltpu.SemaphoreType.DMA
    rows, dm = x.shape[1:]
    return pl.pallas_call(
        functools.partial(gather_kernel, nz, ny, split),
        out_shape=[
            jax.ShapeDtypeStruct((nch, 2, nz, ny, R, C), w.dtype),
            jax.ShapeDtypeStruct((4, rows, dm), x.dtype),
            jax.ShapeDtypeStruct((4, rows, dm), x.dtype),
        ],
        in_specs=[V, V, V],
        out_specs=[V, V, V],
        scratch_shapes=[
            S((nch, nz - 1)),
            S((nch, nz - 1)),
            S((nch, 2, 2)),
            S((nch, 2, 2)),
            S((6,)),
            S((6,)),
            S((2 + nch,)),
        ],
        compiler_params=pltpu.CompilerParams(
            collective_id=0, has_side_effects=True, vmem_limit_bytes=VMEM_LIMIT
        ),
    )(w, x, g)


def settle_kernel(nz, ny, split, *refs):
    grads = refs[:3]
    vec, lo, ig, out, vout, lo_out, ig_out = refs[3:10]
    ra1, ra2, rb1, rb2, r3, s2, vsend, vr, ss, sr, zs, zr, acts, actr, vs, vrs, loc = refs[10:]
    f, t, z, y, xx, c = place(ny)
    nch = 3
    R = out.shape[1]
    xpeer = (f, (1 - xx) * 2 + c)
    ypeer = (z * ny + (1 - y), t)
    cpeer = (f, xx * 2 + 1 - c)
    zp = [((z + d) % nz) * ny + y for d in range(1, nz)]
    greet([xpeer, ypeer, cpeer] + [(q, t) for q in zp])
    other = 1 - xx
    A = pl.ds(0, split)
    B = pl.ds(split, R - split)
    o1 = remote(lo.at[other], lo_out.at[xx], acts.at[0], actr.at[0], xpeer)
    o2 = remote(ig.at[other], ig_out.at[xx], acts.at[1], actr.at[1], xpeer)
    l1 = pltpu.make_async_copy(lo.at[xx], lo_out.at[xx], loc.at[0])
    l2 = pltpu.make_async_copy(ig.at[xx], ig_out.at[xx], loc.at[1])
    v0 = remote(vec, vr.at[0], vs.at[0], vrs.at[0], xpeer)
    v0.start()
    st1 = []
    for ch in range(nch):
        a = remote(grads[ch].at[other, :, :, A], ra1.at[ch], ss.at[ch, 0, 0], sr.at[ch, 0, 0], xpeer)
        b = remote(grads[ch].at[:, :, 1 - y, B], rb1.at[ch], ss.at[ch, 0, 1], sr.at[ch, 0, 1], ypeer)
        a.start()
        b.start()
        st1.append((a, b))
    o1.start()
    o2.start()
    l1.start()
    l2.start()
    st2 = []
    for ch in range(nch):
        a, b = st1[ch]
        a.wait()
        for zi in range(nz):
            ra1[ch, zi, 1 - y] = (
                ra1[ch, zi, 1 - y].astype(F32) + grads[ch][xx, zi, 1 - y, A].astype(F32)
            ).astype(BF)
        a2 = remote(ra1.at[ch, :, 1 - y], ra2.at[ch], ss.at[ch, 1, 0], sr.at[ch, 1, 0], ypeer)
        a2.start()
        b.wait()
        for zi in range(nz):
            rb1[ch, other, zi] = (
                rb1[ch, other, zi].astype(F32) + grads[ch][other, zi, y, B].astype(F32)
            ).astype(BF)
        b2 = remote(rb1.at[ch, other], rb2.at[ch], ss.at[ch, 1, 1], sr.at[ch, 1, 1], xpeer)
        b2.start()
        st2.append((a2, b2))
    v0.wait()
    vsend[0] = vec[...] + vr[0]
    v2 = remote(vsend.at[0], vr.at[2], vs.at[2], vrs.at[2], ypeer)
    v2.start()
    v2.wait()
    vsend[1] = vsend[0] + vr[2]
    vz = []
    for d in range(nz - 1):
        cp = remote(vsend.at[1], vr.at[3 + nz - 2 - d], vs.at[3 + d], vrs.at[3 + nz - 2 - d], (zp[d], t))
        cp.start()
        vz.append(cp)
    st3 = []
    for ch in range(nch):
        a2, b2 = st2[ch]
        a2.wait()
        for zi in range(nz):
            s2[ch, zi, A] = (
                ra1[ch, zi, y].astype(F32) + grads[ch][xx, zi, y, A].astype(F32) + ra2[ch, zi].astype(F32)
            ).astype(BF)
        b2.wait()
        for zi in range(nz):
            s2[ch, zi, B] = (
                rb1[ch, xx, zi].astype(F32) + grads[ch][xx, zi, y, B].astype(F32) + rb2[ch, zi].astype(F32)
            ).astype(BF)
        row = []
        for d in range(nz - 1):
            k = nz - 2 - d
            cp = remote(s2.at[ch, (z + 1 + d) % nz], r3.at[ch, k], zs.at[ch, d], zr.at[ch, k], (zp[d], t))
            cp.start()
            row.append(cp)
        st3.append(row)
    for cp in vz:
        cp.wait()
    total = vsend[1]
    for d in range(nz - 1):
        total = total + vr[3 + d]
    vsend[2] = total
    vout[c] = total
    v1 = remote(vsend.at[2], vout.at[c], vs.at[1], vrs.at[1], cpeer)
    v1.start()
    for ch in range(nch):
        for cp in st3[ch]:
            cp.wait()
        total = s2[ch, z].astype(F32)
        for d in range(nz - 1):
            total = total + r3[ch, d].astype(F32)
        out[ch] = total
    v1.wait()
    o1.wait()
    o2.wait()
    l1.wait()
    l2.wait()


def settle(grads, vec, lo, ig, nf, split):
    ny = 2
    nz = nf // ny
    _, _, _, R, C = grads[0].shape
    nch = 3
    V = pl.BlockSpec(memory_space=pltpu.VMEM)
    S = pltpu.SemaphoreType.DMA
    M = pltpu.VMEM
    return pl.pallas_call(
        functools.partial(settle_kernel, nz, ny, split),
        out_shape=[
            jax.ShapeDtypeStruct((nch, R, C), F32),
            jax.ShapeDtypeStruct((2,) + vec.shape, F32),
            jax.ShapeDtypeStruct(lo.shape, lo.dtype),
            jax.ShapeDtypeStruct(ig.shape, ig.dtype),
        ],
        in_specs=[V] * 6,
        out_specs=[V] * 4,
        scratch_shapes=[
            M((nch, nz, ny, split, C), BF),
            M((nch, nz, split, C), BF),
            M((nch, 2, nz, R - split, C), BF),
            M((nch, nz, R - split, C), BF),
            M((nch, nz - 1, R, C), BF),
            M((nch, nz, R, C), BF),
            M((3,) + vec.shape, F32),
            M((3 + nz - 1,) + vec.shape, F32),
            S((nch, 2, 2)),
            S((nch, 2, 2)),
            S((nch, nz - 1)),
            S((nch, nz - 1)),
            S((2,)),
            S((2,)),
            S((3 + nz - 1,)),
            S((3 + nz - 1,)),
            S((2,)),
        ],
        compiler_params=pltpu.CompilerParams(
            collective_id=1, has_side_effects=True, vmem_limit_bytes=VMEM_LIMIT
        ),
    )(*grads, vec, lo, ig)


def normalize(values, gain, shift):
    center = values - jnp.mean(values, axis=-1, keepdims=True)
    inverse = lax.rsqrt(jnp.mean(center * center, axis=-1, keepdims=True) + EPS)
    unit = center * inverse
    return (unit, inverse, unit * gain + shift)


def normalize_back(grad_rows, unit, inverse, gain):
    scaled = grad_rows * gain
    return inverse * (
        scaled
        - jnp.mean(scaled, axis=-1, keepdims=True)
        - unit * jnp.mean(scaled * unit, axis=-1, keepdims=True)
    )


def lane_mask(head, rows):
    lanes = lax.broadcasted_iota(jnp.int32, (rows, 2 * HEAD_DIM), 1)
    return (lanes // HEAD_DIM) == head


def delayed(v, steps):
    rows = lax.broadcasted_iota(jnp.int32, v.shape, 0)
    return jnp.where(rows >= steps, pltpu.roll(v, steps, 0), 0.0)


def ahead(v, steps):
    n = v.shape[0]
    rows = lax.broadcasted_iota(jnp.int32, v.shape, 0)
    return jnp.where(rows < n - steps, pltpu.roll(v, n - steps, 0), 0.0)


def nt(a, b):
    return lax.dot_general(a, b, (((1,), (1,)), ((), ())), preferred_element_type=F32)


def tn(a, b):
    return lax.dot_general(a, b, (((0,), (0,)), ((), ())), preferred_element_type=F32)


def attend_pair(q, k, v, kern, qm, km, vm, o, lse):
    scale = HEAD_DIM ** (-0.5)
    rows = q.shape[0]
    for src, dst, j in ((q, qm, 0), (k, km, 1), (v, vm, 2)):
        w = kern[3 * j : 3 * j + 3, :]
        val = src[...]
        dst[...] = (w[0:1] * val + w[1:2] * delayed(val, 1) + w[2:3] * delayed(val, 2)).astype(BF)
    zero = jnp.zeros((KBLOCK, 2 * HEAD_DIM), BF)
    for blk in range(rows // KBLOCK):
        rs = pl.ds(blk * KBLOCK, KBLOCK)
        keys = pl.ds(0, (blk + 1) * KBLOCK)
        qb = qm[rs, :]
        parts = []
        for h in range(2):
            mask = lane_mask(h, KBLOCK)
            s = nt(jnp.where(mask, qb, zero), km[keys, :]) * scale
            top = jnp.max(s, axis=-1, keepdims=True)
            e = jnp.exp(s - top)
            total = jnp.sum(e, axis=-1, keepdims=True)
            lse[rs, h : h + 1] = top + jnp.log(total)
            p = (e * (1.0 / total)).astype(BF)
            parts.append(jnp.dot(p, vm[keys, :], preferred_element_type=F32))
        o[rs, :] = jnp.where(lane_mask(0, KBLOCK), parts[0], parts[1]).astype(BF)


def attend_kernel(q, k, v, kern, qm, km, vm, o, lse):
    attend_pair(q, k, v, kern, qm, km, vm, o, lse.at[0])


def attend(q, k, v, kern):
    rows, feats = q.shape
    pairs = feats // 128
    spec = pl.BlockSpec((rows, 128), lambda i: (0, i))
    wide = jax.ShapeDtypeStruct((rows, feats), BF)
    return pl.pallas_call(
        attend_kernel,
        grid=(pairs,),
        out_shape=[wide] * 4 + [jax.ShapeDtypeStruct((pairs, rows, 2), F32)],
        in_specs=[spec] * 3 + [pl.BlockSpec((9, 128), lambda i: (0, i))],
        out_specs=[spec] * 4 + [pl.BlockSpec((1, rows, 2), lambda i: (i, 0, 0))],
        compiler_params=pltpu.CompilerParams(vmem_limit_bytes=40 << 20),
    )(q, k, v, kern)


def attend_back_pair(q, k, v, kern, qm, km, vm, do, lse, dq, dk, dv, taps, gq, gk, gv):
    scale = HEAD_DIM ** (-0.5)
    rows = q.shape[0]
    gk[...] = jnp.zeros_like(gk)
    gv[...] = jnp.zeros_like(gv)
    for blk in range(rows // KBLOCK):
        rs = pl.ds(blk * KBLOCK, KBLOCK)
        nk = (blk + 1) * KBLOCK
        keys = pl.ds(0, nk)
        gqb = None
        for h in range(2):
            mask = lane_mask(h, KBLOCK)
            qb = jnp.where(mask, qm[rs, :], jnp.zeros((), BF))
            dob = jnp.where(mask, do[rs, :], jnp.zeros((), BF))
            pe = jnp.exp(nt(qb, km[keys, :]) * scale - lse[rs, h : h + 1])
            dp = nt(dob, vm[keys, :])
            inner = jnp.sum(pe * dp, axis=-1, keepdims=True)
            ds = (pe * (dp - inner)).astype(BF)
            part = jnp.dot(ds, km[keys, :], preferred_element_type=F32)
            gqb = part if h == 0 else jnp.where(mask, part, gqb)
            gk[keys, :] += tn(ds, qb)
            gv[keys, :] += tn(pe.astype(BF), dob)
        gq[rs, :] = gqb * scale
    gk[...] = gk[...] * scale
    lines = []
    for src, grad, dst, j in ((q, gq, dq, 0), (k, gk, dk, 1), (v, gv, dv, 2)):
        w = kern[3 * j : 3 * j + 3, :]
        val = src[...]
        gr = grad[...]
        dst[...] = (w[0:1] * gr + w[1:2] * ahead(gr, 1) + w[2:3] * ahead(gr, 2)).astype(BF)
        lines.append(jnp.sum(gr * val, axis=0, keepdims=True))
        lines.append(jnp.sum(gr * delayed(val, 1), axis=0, keepdims=True))
        lines.append(jnp.sum(gr * delayed(val, 2), axis=0, keepdims=True))
    taps[...] = jnp.concatenate(lines, axis=0)


def attend_back_kernel(q, k, v, kern, qm, km, vm, do, lse, dq, dk, dv, taps, gq, gk, gv):
    attend_back_pair(q, k, v, kern, qm, km, vm, do, lse.at[0], dq, dk, dv, taps, gq, gk, gv)


def attend_back(q, k, v, kern, qm, km, vm, do, lse):
    rows, feats = q.shape
    pairs = feats // 128
    spec = pl.BlockSpec((rows, 128), lambda i: (0, i))
    wide = jax.ShapeDtypeStruct((rows, feats), BF)
    kspec = pl.BlockSpec((9, 128), lambda i: (0, i))
    return pl.pallas_call(
        attend_back_kernel,
        grid=(pairs,),
        out_shape=[wide] * 3 + [jax.ShapeDtypeStruct((9, feats), F32)],
        in_specs=[spec] * 3
        + [kspec]
        + [spec] * 4
        + [pl.BlockSpec((1, rows, 2), lambda i: (i, 0, 0))],
        out_specs=[spec] * 3 + [kspec],
        scratch_shapes=[pltpu.VMEM((rows, 128), F32)] * 3,
        compiler_params=pltpu.CompilerParams(vmem_limit_bytes=40 << 20),
    )(q, k, v, kern, qm, km, vm, do, lse)


def swap(value):
    n = lax.axis_size("tp")
    return lax.ppermute(value, "tp", [(i, i ^ 1) for i in range(n)])


def local(
    layer_input,
    out_grad,
    ln1_gain,
    ln1_bias,
    w_query,
    w_key,
    w_value,
    conv_query,
    conv_key,
    conv_value,
    w_out,
    ln2_gain,
    ln2_bias,
    w_up,
    up_bias,
    w_down,
    down_bias,
):
    nf = lax.axis_size("fsdp")
    rank = lax.axis_index("tp")
    core = rank % 2
    depth, width = w_query.shape
    units = w_up.shape[1]
    span = layer_input.shape[1]
    rows = 4 * span
    padded = -(-depth // 32) * 32
    split = max(16, padded // 48 * 16)
    pack = jnp.stack(
        [jnp.concatenate([w_query, w_key, w_value, w_out.T], axis=1), w_up, w_down.T]
    )
    if padded != depth:
        pack = jnp.pad(pack, ((0, 0), (0, padded - depth), (0, 0)))
    W, X, G = gather(pack, layer_input, out_grad, nf, split)
    W = W.reshape(3, 2, nf, padded, D)[:, :, :, :depth].reshape(3, 2, D, D)
    x = X.reshape(rows, D).astype(F32)
    g = G.reshape(rows, D)

    def mine(vector, size):
        return jnp.stack(
            [
                lax.dynamic_slice_in_dim(vector, (2 * i + core) * size, size, vector.ndim - 1)
                for i in range(2)
            ],
            axis=-2,
        )

    kern = mine(jnp.concatenate([conv_query, conv_key, conv_value], axis=0), width)
    kern = kern.reshape(9, 2 * width)
    bias_up = mine(up_bias, units)

    def half(value):
        v = value.reshape(2, 2, span, D)
        return (
            lax.dynamic_index_in_dim(v, core, 1, keepdims=False),
            lax.dynamic_index_in_dim(v, 1 - core, 1, keepdims=False),
        )

    unit_one, inverse_one, normed_one = normalize(x, ln1_gain, ln1_bias)
    hidden_one = normed_one.astype(BF)
    feats = 2 * width
    w_qkvo = jnp.stack(
        [
            jnp.concatenate([W[0, j, :, i * width : (i + 1) * width] for j in range(2)], axis=1)
            for i in range(4)
        ]
    )
    projs = [jnp.dot(hidden_one, w_qkvo[i], preferred_element_type=F32) for i in range(3)]
    qm, km, vm, attn_rows, lse = attend(*projs, kern)
    full_o = w_qkvo[3]
    part = jnp.einsum("tc,dc->td", attn_rows, full_o, preferred_element_type=F32).astype(BF)
    resid = x + part.astype(F32) + swap(part).astype(F32)
    unit_two, inverse_two, normed_two = normalize(resid, ln2_gain, ln2_bias)
    hidden_two = normed_two.astype(BF)
    relus, activs = [], []
    y_part = 0.0
    for j in range(2):
        pre = jnp.dot(hidden_two, W[1, j], preferred_element_type=F32) + bias_up[j]
        r = jnp.maximum(pre, 0.0)
        relus.append(r.astype(BF))
        activs.append((r * r).astype(BF))
        y_part = y_part + jnp.einsum("tu,du->td", activs[j], W[2, j], preferred_element_type=F32)
    y_own, y_other = half(y_part.astype(BF))
    resid_own, _ = half(resid)
    layer_out = (
        resid_own + (y_own.astype(F32) + swap(y_other).astype(F32)) + down_bias
    ).astype(BF)
    g32 = g.astype(F32)
    bias_down_grad = jnp.sum(g32, axis=0)
    dh2 = 0.0
    up_grads, down_grads, bias_up_grads = [], [], []
    for j in range(2):
        da = jnp.einsum("td,du->tu", g, W[2, j], preferred_element_type=F32)
        dz = (da * 2.0 * relus[j].astype(F32)).astype(BF)
        bias_up_grads.append(jnp.sum(dz.astype(F32), axis=0))
        down_grads.append(jnp.einsum("td,tu->du", g, activs[j], preferred_element_type=F32).astype(BF))
        up_grads.append(
            jnp.einsum("td,tu->du", hidden_two, dz, preferred_element_type=F32).astype(BF)
        )
        dh2 = dh2 + jnp.einsum("tu,du->td", dz, W[1, j], preferred_element_type=F32)
    dh2 = dh2.astype(BF)
    dh2 = dh2.astype(F32) + swap(dh2).astype(F32)
    gain_two = jnp.sum(dh2 * unit_two, axis=0)
    shift_two = jnp.sum(dh2, axis=0)
    dx1 = g32 + normalize_back(dh2, unit_two, inverse_two, ln2_gain)
    dattn = dx1.astype(BF)
    out_grad_t = jnp.einsum("td,tc->dc", dattn, attn_rows, preferred_element_type=F32).astype(BF)
    dmixed = jnp.einsum("td,dc->tc", dattn, full_o, preferred_element_type=F32).astype(BF)
    *dprojs, taps = attend_back(*projs, kern, qm, km, vm, dmixed, lse)
    dh1 = 0.0
    attn_grads = []
    for i in range(3):
        dv = dprojs[i]
        attn_grads.append(
            jnp.einsum("td,tc->dc", hidden_one, dv, preferred_element_type=F32).astype(BF)
        )
        dh1 = dh1 + jnp.einsum("tc,dc->td", dv, w_qkvo[i], preferred_element_type=F32)
    own, rest = half(dh1.astype(BF))
    dh1 = own.astype(F32) + swap(rest).astype(F32)
    unit_own, _ = half(unit_one)
    inverse_own = lax.dynamic_index_in_dim(
        inverse_one.reshape(2, 2, span, 1), core, 1, keepdims=False
    )
    dx1_own, _ = half(dx1)
    gain_one = jnp.sum(dh1 * unit_own, axis=(0, 1))
    shift_one = jnp.sum(dh1, axis=(0, 1))
    in_grad = (dx1_own + normalize_back(dh1, unit_own, inverse_own, ln1_gain)).astype(BF)
    ch0 = jnp.stack(
        [
            jnp.concatenate(
                [v[:, j * width : (j + 1) * width] for v in attn_grads + [out_grad_t]], axis=1
            )
            for j in range(2)
        ]
    )

    def slabs(v):
        v = v.reshape(2, nf // 2, 2, depth, D)
        if padded != depth:
            v = jnp.pad(v, ((0, 0),) * 3 + ((0, padded - depth), (0, 0)))
        return v

    grads = [slabs(ch0), slabs(jnp.stack(up_grads)), slabs(jnp.stack(down_grads))]

    pieces = [
        taps.reshape(-1),
        *bias_up_grads,
        gain_two,
        shift_two,
        bias_down_grad,
        gain_one,
        shift_one,
    ]
    vec = jnp.concatenate(pieces)
    count = vec.shape[0]
    lines = -(-count // 1024) * 8
    vec = jnp.pad(vec, (0, lines * 128 - count)).reshape(lines, 128)
    out, vec, lo, ig = settle(grads, vec, layer_out, in_grad, nf, split)
    vec = vec.reshape(2, lines * 128)
    at = 9 * feats
    tap_sums = vec[:, :at].reshape(2, 3, 3, 2, width).transpose(1, 2, 3, 0, 4).reshape(3, 3, D)
    up_sums = vec[:, at : at + 2 * units].reshape(2, 2, units).transpose(1, 0, 2).reshape(FF)
    at += 2 * units
    both = [vec[0, at + i * D : at + (i + 1) * D] for i in range(5)]
    ln1_sums = [both[i] + vec[1, at + i * D : at + (i + 1) * D] for i in (3, 4)]
    out = out[:, :depth]
    qg, kg, vg, og = [out[0][:, i * width : (i + 1) * width] for i in range(4)]
    return (
        lo,
        ig,
        ln1_sums[0],
        ln1_sums[1],
        qg,
        kg,
        vg,
        tap_sums[0],
        tap_sums[1],
        tap_sums[2],
        og.T,
        both[0],
        both[1],
        out[1],
        up_sums,
        out[2].T,
        both[2],
    )


def solution(mesh):
    rowsharded = P(None, ("fsdp", "tp"), None)
    return jax.shard_map(
        local,
        mesh=mesh,
        in_specs=(
            rowsharded,
            rowsharded,
            P(),
            P(),
            P("fsdp", "tp"),
            P("fsdp", "tp"),
            P("fsdp", "tp"),
            P(),
            P(),
            P(),
            P("tp", "fsdp"),
            P(),
            P(),
            P("fsdp", "tp"),
            P(),
            P("tp", "fsdp"),
            P(),
        ),
        out_specs=(
            rowsharded,
            rowsharded,
            P(),
            P(),
            P("fsdp", "tp"),
            P("fsdp", "tp"),
            P("fsdp", "tp"),
            P(),
            P(),
            P(),
            P("tp", "fsdp"),
            P(),
            P(),
            P("fsdp", "tp"),
            P(),
            P("tp", "fsdp"),
            P(),
        ),
        check_vma=False,
    )
```
